32 devices in a mesh: krow: 16 (over z, x, core), kcol: 2 (over y).
Axes of the slice: x: 2, y: 2, z: 4, core: 2. Of those that a mesh axis runs over, the one named last changes fastest.
Arguments:
- green: bfloat16 [4, 2, 16, 4, 256, 256], P(None, None, 'krow', 'kcol'), may hold values from -6 to 6
- screened: float32 [16, 4, 65536], P(None, None, ('krow', 'kcol')), may hold values from 0.1 to 1
Outputs:
- sigma: bfloat16 [4, 2, 16, 4, 256, 256], P(None, None, 'krow', 'kcol')
- dressed: bfloat16 [4, 2, 16, 4, 256, 256], P(None, None, 'krow', 'kcol')
The draws below stay inside these ranges and needn't reach their ends.
All inputs are finite; a program needn't handle non-finite values.
Results may differ from the reference program's by a relative error of at most 0.0053.
Values may be sent and summed in bfloat16 or wider, within the bound.
A program may use at most 64 MiB of HBM per device.

```python
import math
import jax
import jax.numpy as jnp
from jax import lax

NO = 256
NE = 4
K1 = 16
K2 = 4
PAIRS = 65536


def block_levels(own_key, dims, cuts, low, largest):
    def one(position, parts):
        draws = jax.random.uniform(jax.random.fold_in(jax.random.fold_in(own_key, 6), position), (parts,), jnp.float32, low / len(cuts), largest / len(cuts))
        return jnp.repeat(jnp.exp(draws), dims[position] // parts).reshape((-1,) + (1,) * (len(dims) - position - 1))

    factor_of = one(*cuts[0])
    for cut in cuts[1:]:
        factor_of = factor_of * one(*cut)
    return factor_of


def noise(stream_key, shape, scale, reach, pieces=(), kind=jnp.bfloat16):
    level = block_levels(stream_key, shape, pieces, -0.22, 0.18) if pieces else 1.0
    array = jax.random.normal(stream_key, shape, jnp.float32) * scale * level
    return jnp.minimum(jnp.maximum(array, -reach), reach).astype(kind)


def setup_inputs(seed: int = 0) -> dict:
    key_of = jax.random.split(jax.random.key(seed), 3)
    return {
        "green": noise(key_of[0], (NE, 2, K1, K2, NO, NO), 1.0, 6.0, ((2, 16), (3, 2))),
        "screened": jnp.clip(0.1 + 0.9 * jax.random.uniform(key_of[1], (K1, K2, PAIRS), jnp.float32) ** block_levels(key_of[1], (K1, K2, PAIRS), ((2, 32),), -0.2, 0.2), 0.1, 1.0),
    }


full_turn = 2.0 * math.pi


def phase_tables(length, forward):
    step_counter = jnp.arange(length, dtype=jnp.int32)
    product = (step_counter[:, None] * step_counter[None, :]) % length
    angles = full_turn * product.astype(jnp.float32) / length
    if forward:
        return jnp.cos(angles) / length, jnp.sin(angles) / length
    return jnp.cos(angles), -jnp.sin(angles)


def apply_over_axis(matrix, values, along_dim):
    letters = "abcdefgh"[:values.ndim]
    target = letters[:along_dim] + "z" + letters[along_dim + 1:]
    formula = "z" + letters[along_dim] + "," + letters + "->" + target
    return jnp.einsum(formula, matrix, values, precision=lax.Precision.HIGHEST)


def complex_along(state, cosine, sine, along_dim):
    real_part, imag_part = state
    out_real = apply_over_axis(cosine, real_part, along_dim) - apply_over_axis(sine, imag_part, along_dim)
    out_imag = apply_over_axis(sine, real_part, along_dim) + apply_over_axis(cosine, imag_part, along_dim)
    return out_real, out_imag


def matmul_batch(left, right):
    return jnp.einsum('xyij,xyjl->xyil', left, right, precision=lax.Precision.HIGHEST)


def reference(green, screened):
    fwd_one = phase_tables(K1, True)
    fwd_two = phase_tables(K2, True)
    inv_one = phase_tables(K1, False)
    inv_two = phase_tables(K2, False)
    pair_weights = screened.reshape(K1, K2, NO, NO)
    green_rows = jnp.moveaxis(green, 4, 0)
    weight_rows = jnp.moveaxis(pair_weights, 2, 0)

    def one_row(operand_list):
        block, wblock = operand_list
        state = (block[:, 0].astype(jnp.float32), block[:, 1].astype(jnp.float32))
        state = complex_along(state, fwd_one[0], fwd_one[1], 1)
        state = complex_along(state, fwd_two[0], fwd_two[1], 2)
        state = (-wblock * state[0], -wblock * state[1])
        state = complex_along(state, inv_one[0], inv_one[1], 1)
        state = complex_along(state, inv_two[0], inv_two[1], 2)
        return jnp.stack(state, 1).astype(jnp.bfloat16)

    sigma = lax.map(one_row, (green_rows, weight_rows))
    sigma = jnp.moveaxis(sigma, 0, 4)

    def one_energy(operand_list):
        green_value_list, self_energy_values = operand_list
        green_real = green_value_list[0].astype(jnp.float32)
        green_imag = green_value_list[1].astype(jnp.float32)
        self_energy_real = self_energy_values[0].astype(jnp.float32)
        self_energy_imaginary = self_energy_values[1].astype(jnp.float32)
        kern_real = matmul_batch(green_real, self_energy_real) - matmul_batch(green_imag, self_energy_imaginary)
        kern_imag = matmul_batch(green_real, self_energy_imaginary) + matmul_batch(green_imag, self_energy_real)
        kern_real = lax.optimization_barrier(kern_real.astype(jnp.bfloat16)).astype(jnp.float32)
        kern_imag = lax.optimization_barrier(kern_imag.astype(jnp.bfloat16)).astype(jnp.float32)
        corr_real = matmul_batch(kern_real, green_real) - matmul_batch(kern_imag, green_imag)
        corr_imag = matmul_batch(kern_real, green_imag) + matmul_batch(kern_imag, green_real)
        return jnp.stack((green_real + corr_real / NO, green_imag + corr_imag / NO), 0).astype(jnp.bfloat16)

    dressed = lax.map(one_energy, (green, sigma))
    return sigma, dressed
```

```python
import functools
import math

import jax
import jax.numpy as jnp
from jax import lax
from jax.experimental import pallas as pl
from jax.experimental.pallas import tpu as pltpu
from jax.sharding import PartitionSpec as P

SUBLANES = 8
LANES = 128


def turn(values, count, size, sign):
    real, imag = values
    count = count * sign % size
    if count * 8 % size == 0:
        eighth = count * 8 // size
        half = math.sqrt(0.5)
        if eighth == 0:
            return real, imag
        if eighth == 2:
            return -imag, real
        if eighth == 4:
            return -real, -imag
        if eighth == 6:
            return imag, -real
        if eighth == 1:
            return (real - imag) * half, (real + imag) * half
        if eighth == 3:
            return (real + imag) * -half, (real - imag) * half
        if eighth == 5:
            return (imag - real) * half, (real + imag) * -half
        return (real + imag) * half, (imag - real) * half
    angle = 2.0 * math.pi * count / size
    cosine, sine = math.cos(angle), math.sin(angle)
    return real * cosine - imag * sine, real * sine + imag * cosine


def transform(values, sign):
    size = len(values)
    if size == 1:
        return values
    if size % 2:
        out = []
        for target in range(size):
            terms = [turn(v, target * source, size, sign) for source, v in enumerate(values)]
            out.append((sum(t[0] for t in terms), sum(t[1] for t in terms)))
        return out
    even = transform(values[0::2], sign)
    odd = transform(values[1::2], sign)
    low, high = [], []
    for t in range(size // 2):
        real, imag = turn(odd[t], t, size, sign)
        low.append((even[t][0] + real, even[t][1] + imag))
        high.append((even[t][0] - real, even[t][1] - imag))
    return low + high


CORES = 2
SPLIT_X = 2


def corrected(g_real, g_imag, s_real, s_imag):
    def times(left, right):
        return jnp.dot(left, right, preferred_element_type=jnp.float32)

    kern_real = (times(g_real, s_real) - times(g_imag, s_imag)).astype(jnp.bfloat16)
    kern_imag = (times(g_real, s_imag) + times(g_imag, s_real)).astype(jnp.bfloat16)
    corr_real = times(kern_real, g_real) - times(kern_imag, g_imag)
    corr_imag = times(kern_real, g_imag) + times(kern_imag, g_real)
    share = 1.0 / g_real.shape[-1]
    return (
        (g_real.astype(jnp.float32) + corr_real * share).astype(jnp.bfloat16),
        (g_imag.astype(jnp.float32) + corr_imag * share).astype(jnp.bfloat16),
    )


def kernel(
    grid_dims, mesh_dims, rows,
    green_far, weights_far, green, sigma, dressed,
    weights, arrived, results, middle, pair_weights,
    load_sems, out_sems, in_sems, back_out_sems, back_in_sems, near_sems, all_in,
):
    one, two = grid_dims
    row_count, column_count = mesh_dims
    devices = row_count * column_count
    energies, _, local, orbitals, _ = green.shape
    local_one, local_two = one // row_count, two // column_count
    my_row, my_column = lax.axis_index("krow"), lax.axis_index("kcol")
    me = my_row * column_count + my_column

    plane_rows = SPLIT_X * CORES
    layers = row_count // plane_rows
    half = layers // 2
    plane = plane_rows * column_count
    pillars = SPLIT_X * column_count
    z = lax.div(my_row, plane_rows)
    x = lax.rem(lax.div(my_row, CORES), SPLIT_X)
    core = lax.rem(my_row, CORES)
    y = my_column
    pillar = x * column_count + y

    def at_place(z_, x_, core_, y_):
        return ((z_ * SPLIT_X + x_) * CORES + core_, y_)

    def flat_of(place):
        return place[0] * column_count + place[1]

    def signal(sem, place):
        pl.semaphore_signal(
            sem, inc=1, device_id=place, device_id_type=pl.DeviceIdType.MESH
        )

    def strip(owner):
        return pl.ds(pl.multiple_of(owner * rows, rows), rows)

    def load(e):
        return pltpu.make_async_copy(green_far.at[e], green.at[e], load_sems.at[e])

    load_weights = pltpu.make_async_copy(weights_far, weights, load_sems.at[energies])

    barrier = pltpu.get_barrier_semaphore()
    last_place = (z == layers - 1) & (x == SPLIT_X - 1) & (y == column_count - 1)

    @pl.when(last_place)
    def _():
        signal(barrier, at_place(z, x, 1 - core, y))

    def flag(condition):
        return jnp.where(condition, 1, 0)

    heard = CORES * (flag(x > 0) + flag(y > 0) + flag(z > 0)) + flag(last_place) * (CORES - 1)

    @pl.when(heard > 0)
    def _():
        pl.semaphore_wait(barrier, heard)

    for c in range(CORES):
        @pl.when(z < layers - 1)
        def _():
            signal(barrier, at_place(z + 1, x, c, y))

        @pl.when(z >= half)
        def _():
            signal(near_sems.at[z - half], at_place(half - 1, x, c, y))

        @pl.when(x < SPLIT_X - 1)
        def _():
            signal(barrier, at_place(z, x + 1, c, y))

        @pl.when(y < column_count - 1)
        def _():
            signal(barrier, at_place(z, x, c, y + 1))

    @pl.when(last_place)
    def _():
        @pl.loop(1, row_count // CORES * column_count)
        def _(step):
            chip = row_count // CORES * column_count - 1 - step
            signal(all_in, (lax.div(chip, column_count) * CORES + core, lax.rem(chip, column_count)))

    def send(e, place):
        peer = flat_of(place)
        pltpu.make_async_remote_copy(
            src_ref=green_far.at[e, :, :, strip(peer), :],
            dst_ref=arrived.at[e, me],
            send_sem=out_sems.at[e],
            recv_sem=in_sems.at[e],
            device_id=place,
            device_id_type=pl.DeviceIdType.MESH,
        ).start()

    def send_pillar(z_):
        @pl.loop(0, energies)
        def _(e):
            for c in range(CORES):
                send(e, at_place(z_, x, lax.rem(core + c, CORES), y))

    @pl.when(z == half)
    def _():
        @pl.loop(0, half)
        def _(step):
            send_pillar(half - 1 - step)

    for e in range(energies):
        load(e).start()
    load_weights.start()

    @pl.when(z == half - 1)
    def _():
        @pl.loop(0, layers - half)
        def _(step):
            pl.semaphore_wait(near_sems.at[step], CORES)
            send_pillar(half + step)

    @pl.when(jnp.logical_not(last_place))
    def _():
        pl.semaphore_wait(all_in, 1)

    middle_layer = (z == half) | (z == half - 1)

    def each_peer(first_round, body):
        @pl.loop(0, pillars)
        def _(turn_):
            to = lax.rem(pillar + 1 + turn_, pillars)
            own = turn_ == pillars - 1

            @pl.loop(0, layers)
            def _(step):
                z_ = lax.rem(z + step, layers)
                across = (z_ >= half) != (z >= half)
                done = flag(own & (step == 0))
                if first_round:
                    done = jnp.where(own & middle_layer & across, CORES, done)

                @pl.loop(done, CORES)
                def _(c):
                    body(at_place(
                        z_, lax.div(to, column_count), lax.rem(core + c, CORES),
                        lax.rem(to, column_count),
                    ))

    @pl.loop(0, energies)
    def _(e):
        each_peer(True, lambda place: send(e, place))

    def wait_all(part, sem):
        pltpu.make_async_copy(part, part, sem).wait()

    def others(buffer, e):
        return buffer.at[e, pl.ds(0, devices - 1)]

    def slot(k1, k2):
        return (
            (k1 // local_one) * column_count + k2 // local_two,
            (k1 % local_one) * local_two + k2 % local_two,
        )

    scale = -1.0 / (one * two)
    load_weights.wait()

    @pl.loop(0, one)
    def _(r1):
        for r2 in range(two):
            for row in range(rows):
                part = weights[r1, r2:r2 + 1, row * orbitals:(row + 1) * orbitals]
                pair_weights[r1, r2, row:row + 1, :] = part * scale

    def transform_energy(e):
        load(e).wait()
        wait_all(others(arrived, e), in_sems.at[e])
        arrived[e, me] = green[e, :, :, strip(me), :]

        @pl.loop(0, orbitals // LANES)
        def _(h):
            lanes = pl.ds(pl.multiple_of(h * LANES, LANES), LANES)
            for k2 in range(two):
                values = []
                for k1 in range(one):
                    s, at = slot(k1, k2)
                    values.append(tuple(
                        arrived[e, s, c, at, :, lanes].astype(jnp.float32) for c in range(2)
                    ))
                for r1, v in enumerate(transform(values, 1)):
                    middle[r1, k2, 0] = v[0]
                    middle[r1, k2, 1] = v[1]
            for r1 in range(one):
                values = transform([(middle[r1, k2, 0], middle[r1, k2, 1]) for k2 in range(two)], 1)
                for r2 in range(two):
                    weight = pair_weights[r1, r2, :, lanes]
                    values[r2] = (values[r2][0] * weight, values[r2][1] * weight)
                for k2, v in enumerate(transform(values, -1)):
                    middle[r1, k2, 0] = v[0]
                    middle[r1, k2, 1] = v[1]
            for k2 in range(two):
                values = [(middle[r1, k2, 0], middle[r1, k2, 1]) for r1 in range(one)]
                for k1, v in enumerate(transform(values, -1)):
                    s, at = slot(k1, k2)
                    for c in range(2):
                        results[e, s, c, at, :, lanes] = v[c].astype(jnp.bfloat16)

    def send_back(e):
        def one_send(place):
            pltpu.make_async_remote_copy(
                src_ref=results.at[e, flat_of(place)],
                dst_ref=sigma.at[e, :, :, strip(me), :],
                send_sem=back_out_sems.at[e],
                recv_sem=back_in_sems.at[e],
                device_id=place,
                device_id_type=pl.DeviceIdType.MESH,
            ).start()

        each_peer(False, one_send)

    last = energies - 1

    @pl.loop(0, energies)
    def _(e):
        transform_energy(e)

        send_back(e)
        sigma[e, :, :, strip(me), :] = results[e, me]

    @pl.loop(0, last)
    def _(e):
        wait_all(others(results, e), back_in_sems.at[e])

        @pl.loop(0, local)
        def _(at):
            real, imag = corrected(
                green[e, 0, at], green[e, 1, at], sigma[e, 0, at], sigma[e, 1, at]
            )
            dressed[e, 0, at] = real
            dressed[e, 1, at] = imag

    @pl.loop(0, last)
    def _(e):
        wait_all(others(arrived, e), out_sems.at[e])
        wait_all(others(results, e), back_out_sems.at[e])

    wait_all(others(arrived, last), out_sems.at[last])
    wait_all(others(results, last), back_out_sems.at[last])
    wait_all(others(results, last), back_in_sems.at[last])


def finish(green, sigma, dressed, sigma_far, dressed_far, piece, sems):
    energies, _, local, _, _ = green.shape
    last = energies - 1
    copies = [
        pltpu.make_async_copy(sigma, sigma_far, sems.at[local]),
        pltpu.make_async_copy(
            dressed.at[pl.ds(0, last)], dressed_far.at[pl.ds(0, last)], sems.at[local + 1]
        ),
    ]
    for copy in copies:
        copy.start()
    for at in range(local):
        piece[at, 0], piece[at, 1] = corrected(
            green[last, 0, at], green[last, 1, at], sigma[last, 0, at], sigma[last, 1, at]
        )
        copies.append(
            pltpu.make_async_copy(piece.at[at], dressed_far.at[last, :, at], sems.at[at])
        )
        copies[-1].start()
    for copy in copies:
        copy.wait()


def exchange_in_kernel(green, screened):
    mesh_dims = (lax.axis_size("krow"), lax.axis_size("kcol"))
    devices = mesh_dims[0] * mesh_dims[1]
    energies, _, local_one, local_two, orbitals, _ = green.shape
    grid_dims = screened.shape[:2]
    rows = orbitals // devices
    local = local_one * local_two
    layers = mesh_dims[0] // (SPLIT_X * CORES)
    flat = (energies, 2, local, orbitals, orbitals)
    block = (energies, devices, 2, local, rows, orbitals)
    vmem = pl.BlockSpec(memory_space=pltpu.VMEM)
    far = pl.BlockSpec(memory_space=pltpu.HBM)
    held = pl.pallas_call(
        functools.partial(kernel, grid_dims, mesh_dims, rows),
        out_shape=[pltpu.VMEM(flat, jnp.bfloat16)] * 3,
        in_specs=[far, far],
        out_specs=[vmem] * 3,
        scratch_shapes=[
            pltpu.VMEM(screened.shape, jnp.float32),
            pltpu.VMEM(block, jnp.bfloat16),
            pltpu.VMEM(block, jnp.bfloat16),
            pltpu.VMEM(grid_dims + (2, rows, LANES), jnp.float32),
            pltpu.VMEM(grid_dims + (rows, orbitals), jnp.float32),
            pltpu.SemaphoreType.DMA((energies + 1,)),
            pltpu.SemaphoreType.DMA((energies,)),
            pltpu.SemaphoreType.DMA((energies,)),
            pltpu.SemaphoreType.DMA((energies,)),
            pltpu.SemaphoreType.DMA((energies,)),
            pltpu.SemaphoreType.REGULAR((layers - layers // 2,)),
            pltpu.SemaphoreType.REGULAR,
        ],
        compiler_params=pltpu.CompilerParams(
            collective_id=0, has_side_effects=True, vmem_limit_bytes=15 * math.prod(block)
        ),
    )(*(
        pltpu.with_memory_space_constraint(v, pltpu.HBM) for v in (green.reshape(flat), screened)
    ))
    sigma, dressed = pl.pallas_call(
        finish,
        out_shape=[jax.ShapeDtypeStruct(flat, jnp.bfloat16)] * 2,
        in_specs=[vmem] * 3,
        out_specs=[far] * 2,
        scratch_shapes=[
            pltpu.VMEM((local, 2, orbitals, orbitals), jnp.bfloat16),
            pltpu.SemaphoreType.DMA((local + 2,)),
        ],
        compiler_params=pltpu.CompilerParams(vmem_limit_bytes=8 * math.prod(block)),
    )(*held)
    return sigma.reshape(green.shape), dressed.reshape(green.shape)


full_turn = 2.0 * math.pi


def phase_tables(length, forward):
    step_counter = jnp.arange(length, dtype=jnp.int32)
    product = step_counter[:, None] * step_counter[None, :] % length
    angles = full_turn * product.astype(jnp.float32) / length
    if forward:
        return (jnp.cos(angles) / length, jnp.sin(angles) / length)
    return (jnp.cos(angles), -jnp.sin(angles))


def apply_over_axis(matrix, values, along_dim):
    letters = "abcdefgh"[: values.ndim]
    target = letters[:along_dim] + "z" + letters[along_dim + 1 :]
    formula = "z" + letters[along_dim] + "," + letters + "->" + target
    return jnp.einsum(formula, matrix, values, precision=lax.Precision.HIGHEST)


def complex_along(state, cosine, sine, along_dim):
    real_part, imag_part = state
    out_real = apply_over_axis(cosine, real_part, along_dim) - apply_over_axis(
        sine, imag_part, along_dim
    )
    out_imag = apply_over_axis(sine, real_part, along_dim) + apply_over_axis(
        cosine, imag_part, along_dim
    )
    return (out_real, out_imag)


def weigh_back(state, weights, lead_one, lead_two):
    state = (-weights * state[0], -weights * state[1])
    cos_one, sin_one = phase_tables(lead_one, False)
    state = complex_along(state, cos_one, sin_one, 1)
    cos_two, sin_two = phase_tables(lead_two, False)
    state = complex_along(state, cos_two, sin_two, 2)
    return jnp.stack(state, 1).astype(jnp.bfloat16)


def whole_local(pieces, weights):
    state = (pieces[:, 0].astype(jnp.float32), pieces[:, 1].astype(jnp.float32))
    cos_two, sin_two = phase_tables(pieces.shape[3], True)
    state = complex_along(state, cos_two, sin_two, 2)
    cos_one, sin_one = phase_tables(pieces.shape[2], True)
    state = complex_along(state, cos_one, sin_one, 1)
    return weigh_back(state, weights, pieces.shape[2], pieces.shape[3])


def matmul_batch(left, right):
    return jnp.einsum("eklij,ekljm->eklim", left, right, preferred_element_type=jnp.float32)


def per_device(green, screened):
    krow_count = lax.axis_size("krow")
    momentum_column_count = lax.axis_size("kcol")
    orbitals = green.shape[4]
    slice_len = orbitals * green.shape[5] // (krow_count * momentum_column_count)
    blocks = green.reshape(green.shape[:4] + (krow_count, momentum_column_count, slice_len))
    weights = screened.reshape(screened.shape[0], screened.shape[1], 1, 1, screened.shape[2])
    gathered = lax.all_to_all(
        lax.all_to_all(blocks, "krow", split_axis=4, concat_axis=2, tiled=True),
        "kcol",
        split_axis=5,
        concat_axis=3,
        tiled=True,
    )
    middle = whole_local(gathered, weights)
    partway = lax.all_to_all(middle, "krow", split_axis=2, concat_axis=4, tiled=True)
    returned = lax.all_to_all(partway, "kcol", split_axis=3, concat_axis=5, tiled=True)
    sigma = returned.reshape(green.shape)
    green_real = green[:, 0]
    green_imag = green[:, 1]
    self_energy_real = sigma[:, 0]
    self_energy_imaginary = sigma[:, 1]
    kern_real = (
        matmul_batch(green_real, self_energy_real) - matmul_batch(green_imag, self_energy_imaginary)
    ).astype(jnp.bfloat16)
    kern_imag = (
        matmul_batch(green_real, self_energy_imaginary) + matmul_batch(green_imag, self_energy_real)
    ).astype(jnp.bfloat16)
    corr_real = matmul_batch(kern_real, green_real) - matmul_batch(kern_imag, green_imag)
    corr_imag = matmul_batch(kern_real, green_imag) + matmul_batch(kern_imag, green_real)
    dressed_real = green_real.astype(jnp.float32) + corr_real / orbitals
    dressed_imag = green_imag.astype(jnp.float32) + corr_imag / orbitals
    dressed = jnp.stack((dressed_real, dressed_imag), 1).astype(jnp.bfloat16)
    return (sigma, dressed)


def choose(green, screened):
    devices = lax.axis_size("krow") * lax.axis_size("kcol")
    orbitals = green.shape[4]
    shaped = lax.axis_size("krow") % (2 * SPLIT_X * CORES) == 0 and lax.axis_size("kcol") > 1
    if shaped and orbitals % (devices * SUBLANES) == 0 and orbitals % LANES == 0:
        return exchange_in_kernel(green, screened)
    return per_device(green, screened)


def solution(mesh):
    placed = (P(None, None, "krow", "kcol", None, None), P(None, None, ("krow", "kcol")))
    return jax.shard_map(
        choose,
        mesh=mesh,
        in_specs=placed,
        out_specs=(
            P(None, None, "krow", "kcol", None, None),
            P(None, None, "krow", "kcol", None, None),
        ),
        check_vma=False,
    )
```

```python
import functools
import math

import jax
import jax.numpy as jnp
from jax import lax
from jax.experimental import pallas as pl
from jax.experimental.pallas import tpu as pltpu
from jax.sharding import PartitionSpec as P

SUBLANES = 8
LANES = 128


def turn(values, count, size, sign):
    real, imag = values
    count = count * sign % size
    if count * 8 % size == 0:
        eighth = count * 8 // size
        half = math.sqrt(0.5)
        if eighth == 0:
            return real, imag
        if eighth == 2:
            return -imag, real
        if eighth == 4:
            return -real, -imag
        if eighth == 6:
            return imag, -real
        if eighth == 1:
            return (real - imag) * half, (real + imag) * half
        if eighth == 3:
            return (real + imag) * -half, (real - imag) * half
        if eighth == 5:
            return (imag - real) * half, (real + imag) * -half
        return (real + imag) * half, (imag - real) * half
    angle = 2.0 * math.pi * count / size
    cosine, sine = math.cos(angle), math.sin(angle)
    return real * cosine - imag * sine, real * sine + imag * cosine


def transform(values, sign):
    size = len(values)
    if size == 1:
        return values
    if size % 2:
        out = []
        for target in range(size):
            terms = [turn(v, target * source, size, sign) for source, v in enumerate(values)]
            out.append((sum(t[0] for t in terms), sum(t[1] for t in terms)))
        return out
    even = transform(values[0::2], sign)
    odd = transform(values[1::2], sign)
    low, high = [], []
    for t in range(size // 2):
        real, imag = turn(odd[t], t, size, sign)
        low.append((even[t][0] + real, even[t][1] + imag))
        high.append((even[t][0] - real, even[t][1] - imag))
    return low + high


CORES = 2
SPLIT_X = 2
PILLAR_ORDER = ((1, 0, 2, 3), (2, 0, 3, 1), (0, 1, 3, 2), (0, 2, 1, 3))


def corrected(g_real, g_imag, s_real, s_imag):
    def times(left, right):
        return jnp.dot(left, right, preferred_element_type=jnp.float32)

    kern_real = (times(g_real, s_real) - times(g_imag, s_imag)).astype(jnp.bfloat16)
    kern_imag = (times(g_real, s_imag) + times(g_imag, s_real)).astype(jnp.bfloat16)
    corr_real = times(kern_real, g_real) - times(kern_imag, g_imag)
    corr_imag = times(kern_real, g_imag) + times(kern_imag, g_real)
    share = 1.0 / g_real.shape[-1]
    return (
        (g_real.astype(jnp.float32) + corr_real * share).astype(jnp.bfloat16),
        (g_imag.astype(jnp.float32) + corr_imag * share).astype(jnp.bfloat16),
    )


def kernel(
    grid_dims, mesh_dims, rows,
    green_far, weights_far, green, sigma, dressed,
    weights, arrived, results, middle, pair_weights,
    load_sems, out_sems, in_sems, back_out_sems, back_in_sems, near_sems, all_in,
):
    one, two = grid_dims
    row_count, column_count = mesh_dims
    devices = row_count * column_count
    energies, _, local, orbitals, _ = green.shape
    local_one, local_two = one // row_count, two // column_count
    my_row, my_column = lax.axis_index("krow"), lax.axis_index("kcol")
    me = my_row * column_count + my_column

    plane_rows = SPLIT_X * CORES
    layers = row_count // plane_rows
    half = layers // 2
    plane = plane_rows * column_count
    pillars = SPLIT_X * column_count
    z = lax.div(my_row, plane_rows)
    x = lax.rem(lax.div(my_row, CORES), SPLIT_X)
    core = lax.rem(my_row, CORES)
    y = my_column
    pillar = x * column_count + y

    def at_place(z_, x_, core_, y_):
        return ((z_ * SPLIT_X + x_) * CORES + core_, y_)

    def flat_of(place):
        return place[0] * column_count + place[1]

    def signal(sem, place):
        pl.semaphore_signal(
            sem, inc=1, device_id=place, device_id_type=pl.DeviceIdType.MESH
        )

    def strip(owner):
        return pl.ds(pl.multiple_of(owner * rows, rows), rows)

    def load(e):
        return pltpu.make_async_copy(green_far.at[e], green.at[e], load_sems.at[e])

    load_weights = pltpu.make_async_copy(weights_far, weights, load_sems.at[energies])

    barrier = pltpu.get_barrier_semaphore()
    last_place = (z == layers - 1) & (x == SPLIT_X - 1) & (y == column_count - 1)

    @pl.when(last_place)
    def _():
        signal(barrier, at_place(z, x, 1 - core, y))

    def flag(condition):
        return jnp.where(condition, 1, 0)

    heard = CORES * (flag(x > 0) + flag(y > 0) + flag(z > 0)) + flag(last_place) * (CORES - 1)

    @pl.when(heard > 0)
    def _():
        pl.semaphore_wait(barrier, heard)

    for c in range(CORES):
        @pl.when(z < layers - 1)
        def _():
            signal(barrier, at_place(z + 1, x, c, y))

        @pl.when(z >= half)
        def _():
            signal(near_sems.at[z - half], at_place(half - 1, x, c, y))

        @pl.when(x < SPLIT_X - 1)
        def _():
            signal(barrier, at_place(z, x + 1, c, y))

        @pl.when(y < column_count - 1)
        def _():
            signal(barrier, at_place(z, x, c, y + 1))

    @pl.when(last_place)
    def _():
        @pl.loop(1, row_count // CORES * column_count)
        def _(step):
            chip = row_count // CORES * column_count - 1 - step
            signal(all_in, (lax.div(chip, column_count) * CORES + core, lax.rem(chip, column_count)))

    def send(e, place):
        peer = flat_of(place)
        pltpu.make_async_remote_copy(
            src_ref=green_far.at[e, :, :, strip(peer), :],
            dst_ref=arrived.at[e, me],
            send_sem=out_sems.at[e],
            recv_sem=in_sems.at[e],
            device_id=place,
            device_id_type=pl.DeviceIdType.MESH,
        ).start()

    def send_pillar(z_):
        @pl.loop(0, energies)
        def _(e):
            for c in range(CORES):
                send(e, at_place(z_, x, lax.rem(core + c, CORES), y))

    @pl.when(z == half)
    def _():
        @pl.loop(0, half)
        def _(step):
            send_pillar(half - 1 - step)

    for e in range(energies):
        load(e).start()
    load_weights.start()

    @pl.when(z == half - 1)
    def _():
        @pl.loop(0, layers - half)
        def _(step):
            pl.semaphore_wait(near_sems.at[step], CORES)
            send_pillar(half + step)

    @pl.when(jnp.logical_not(last_place))
    def _():
        pl.semaphore_wait(all_in, 1)

    middle_layer = (z == half) | (z == half - 1)

    def next_pillar(turn_):
        if pillars != len(PILLAR_ORDER):
            return lax.rem(pillar + 1 + turn_, pillars)
        to = 0
        for source, order in enumerate(PILLAR_ORDER):
            for when, target_ in enumerate(order):
                to = to + jnp.where((pillar == source) & (turn_ == when), target_, 0)
        return to

    def each_peer(first_round, body):
        @pl.loop(0, pillars)
        def _(turn_):
            to = next_pillar(turn_)
            own = to == pillar

            @pl.loop(0, layers)
            def _(step):
                z_ = lax.rem(z + step, layers)
                across = (z_ >= half) != (z >= half)
                done = flag(own & (step == 0))
                if first_round:
                    done = jnp.where(own & middle_layer & across, CORES, done)

                @pl.loop(done, CORES)
                def _(c):
                    body(at_place(
                        z_, lax.div(to, column_count), lax.rem(core + c, CORES),
                        lax.rem(to, column_count),
                    ))

    @pl.loop(0, energies)
    def _(e):
        each_peer(True, lambda place: send(e, place))

    def wait_all(part, sem):
        pltpu.make_async_copy(part, part, sem).wait()

    def others(buffer, e):
        return buffer.at[e, pl.ds(0, devices - 1)]

    def slot(k1, k2):
        return (
            (k1 // local_one) * column_count + k2 // local_two,
            (k1 % local_one) * local_two + k2 % local_two,
        )

    scale = -1.0 / (one * two)
    load_weights.wait()

    @pl.loop(0, one)
    def _(r1):
        for r2 in range(two):
            for row in range(rows):
                part = weights[r1, r2:r2 + 1, row * orbitals:(row + 1) * orbitals]
                pair_weights[r1, r2, row:row + 1, :] = part * scale

    def transform_energy(e):
        load(e).wait()
        wait_all(others(arrived, e), in_sems.at[e])
        arrived[e, me] = green[e, :, :, strip(me), :]

        @pl.loop(0, orbitals // LANES)
        def _(h):
            lanes = pl.ds(pl.multiple_of(h * LANES, LANES), LANES)
            for k2 in range(two):
                values = []
                for k1 in range(one):
                    s, at = slot(k1, k2)
                    values.append(tuple(
                        arrived[e, s, c, at, :, lanes].astype(jnp.float32) for c in range(2)
                    ))
                for r1, v in enumerate(transform(values, 1)):
                    middle[r1, k2, 0] = v[0]
                    middle[r1, k2, 1] = v[1]
            for r1 in range(one):
                values = transform([(middle[r1, k2, 0], middle[r1, k2, 1]) for k2 in range(two)], 1)
                for r2 in range(two):
                    weight = pair_weights[r1, r2, :, lanes]
                    values[r2] = (values[r2][0] * weight, values[r2][1] * weight)
                for k2, v in enumerate(transform(values, -1)):
                    middle[r1, k2, 0] = v[0]
                    middle[r1, k2, 1] = v[1]
            for k2 in range(two):
                values = [(middle[r1, k2, 0], middle[r1, k2, 1]) for r1 in range(one)]
                for k1, v in enumerate(transform(values, -1)):
                    s, at = slot(k1, k2)
                    for c in range(2):
                        results[e, s, c, at, :, lanes] = v[c].astype(jnp.bfloat16)

    def send_back(e):
        def one_send(place):
            pltpu.make_async_remote_copy(
                src_ref=results.at[e, flat_of(place)],
                dst_ref=sigma.at[e, :, :, strip(me), :],
                send_sem=back_out_sems.at[e],
                recv_sem=back_in_sems.at[e],
                device_id=place,
                device_id_type=pl.DeviceIdType.MESH,
            ).start()

        each_peer(False, one_send)

    last = energies - 1

    @pl.loop(0, energies)
    def _(e):
        transform_energy(e)

        send_back(e)
        sigma[e, :, :, strip(me), :] = results[e, me]

    @pl.loop(0, last)
    def _(e):
        wait_all(others(results, e), back_in_sems.at[e])

        @pl.loop(0, local)
        def _(at):
            real, imag = corrected(
                green[e, 0, at], green[e, 1, at], sigma[e, 0, at], sigma[e, 1, at]
            )
            dressed[e, 0, at] = real
            dressed[e, 1, at] = imag

    @pl.loop(0, last)
    def _(e):
        wait_all(others(arrived, e), out_sems.at[e])
        wait_all(others(results, e), back_out_sems.at[e])

    wait_all(others(arrived, last), out_sems.at[last])
    wait_all(others(results, last), back_out_sems.at[last])
    wait_all(others(results, last), back_in_sems.at[last])


def finish(green, sigma, dressed, sigma_far, dressed_far, piece, sems):
    energies, _, local, _, _ = green.shape
    last = energies - 1
    copies = [
        pltpu.make_async_copy(sigma, sigma_far, sems.at[local]),
        pltpu.make_async_copy(
            dressed.at[pl.ds(0, last)], dressed_far.at[pl.ds(0, last)], sems.at[local + 1]
        ),
    ]
    for copy in copies:
        copy.start()
    for at in range(local):
        piece[at, 0], piece[at, 1] = corrected(
            green[last, 0, at], green[last, 1, at], sigma[last, 0, at], sigma[last, 1, at]
        )
        copies.append(
            pltpu.make_async_copy(piece.at[at], dressed_far.at[last, :, at], sems.at[at])
        )
        copies[-1].start()
    for copy in copies:
        copy.wait()


def exchange_in_kernel(green, screened):
    mesh_dims = (lax.axis_size("krow"), lax.axis_size("kcol"))
    devices = mesh_dims[0] * mesh_dims[1]
    energies, _, local_one, local_two, orbitals, _ = green.shape
    grid_dims = screened.shape[:2]
    rows = orbitals // devices
    local = local_one * local_two
    layers = mesh_dims[0] // (SPLIT_X * CORES)
    flat = (energies, 2, local, orbitals, orbitals)
    block = (energies, devices, 2, local, rows, orbitals)
    vmem = pl.BlockSpec(memory_space=pltpu.VMEM)
    far = pl.BlockSpec(memory_space=pltpu.HBM)
    held = pl.pallas_call(
        functools.partial(kernel, grid_dims, mesh_dims, rows),
        out_shape=[pltpu.VMEM(flat, jnp.bfloat16)] * 3,
        in_specs=[far, far],
        out_specs=[vmem] * 3,
        scratch_shapes=[
            pltpu.VMEM(screened.shape, jnp.float32),
            pltpu.VMEM(block, jnp.bfloat16),
            pltpu.VMEM(block, jnp.bfloat16),
            pltpu.VMEM(grid_dims + (2, rows, LANES), jnp.float32),
            pltpu.VMEM(grid_dims + (rows, orbitals), jnp.float32),
            pltpu.SemaphoreType.DMA((energies + 1,)),
            pltpu.SemaphoreType.DMA((energies,)),
            pltpu.SemaphoreType.DMA((energies,)),
            pltpu.SemaphoreType.DMA((energies,)),
            pltpu.SemaphoreType.DMA((energies,)),
            pltpu.SemaphoreType.REGULAR((layers - layers // 2,)),
            pltpu.SemaphoreType.REGULAR,
        ],
        compiler_params=pltpu.CompilerParams(
            collective_id=0, has_side_effects=True, vmem_limit_bytes=15 * math.prod(block)
        ),
    )(*(
        pltpu.with_memory_space_constraint(v, pltpu.HBM) for v in (green.reshape(flat), screened)
    ))
    sigma, dressed = pl.pallas_call(
        finish,
        out_shape=[jax.ShapeDtypeStruct(flat, jnp.bfloat16)] * 2,
        in_specs=[vmem] * 3,
        out_specs=[far] * 2,
        scratch_shapes=[
            pltpu.VMEM((local, 2, orbitals, orbitals), jnp.bfloat16),
            pltpu.SemaphoreType.DMA((local + 2,)),
        ],
        compiler_params=pltpu.CompilerParams(vmem_limit_bytes=8 * math.prod(block)),
    )(*held)
    return sigma.reshape(green.shape), dressed.reshape(green.shape)


full_turn = 2.0 * math.pi


def phase_tables(length, forward):
    step_counter = jnp.arange(length, dtype=jnp.int32)
    product = step_counter[:, None] * step_counter[None, :] % length
    angles = full_turn * product.astype(jnp.float32) / length
    if forward:
        return (jnp.cos(angles) / length, jnp.sin(angles) / length)
    return (jnp.cos(angles), -jnp.sin(angles))


def apply_over_axis(matrix, values, along_dim):
    letters = "abcdefgh"[: values.ndim]
    target = letters[:along_dim] + "z" + letters[along_dim + 1 :]
    formula = "z" + letters[along_dim] + "," + letters + "->" + target
    return jnp.einsum(formula, matrix, values, precision=lax.Precision.HIGHEST)


def complex_along(state, cosine, sine, along_dim):
    real_part, imag_part = state
    out_real = apply_over_axis(cosine, real_part, along_dim) - apply_over_axis(
        sine, imag_part, along_dim
    )
    out_imag = apply_over_axis(sine, real_part, along_dim) + apply_over_axis(
        cosine, imag_part, along_dim
    )
    return (out_real, out_imag)


def weigh_back(state, weights, lead_one, lead_two):
    state = (-weights * state[0], -weights * state[1])
    cos_one, sin_one = phase_tables(lead_one, False)
    state = complex_along(state, cos_one, sin_one, 1)
    cos_two, sin_two = phase_tables(lead_two, False)
    state = complex_along(state, cos_two, sin_two, 2)
    return jnp.stack(state, 1).astype(jnp.bfloat16)


def whole_local(pieces, weights):
    state = (pieces[:, 0].astype(jnp.float32), pieces[:, 1].astype(jnp.float32))
    cos_two, sin_two = phase_tables(pieces.shape[3], True)
    state = complex_along(state, cos_two, sin_two, 2)
    cos_one, sin_one = phase_tables(pieces.shape[2], True)
    state = complex_along(state, cos_one, sin_one, 1)
    return weigh_back(state, weights, pieces.shape[2], pieces.shape[3])


def matmul_batch(left, right):
    return jnp.einsum("eklij,ekljm->eklim", left, right, preferred_element_type=jnp.float32)


def per_device(green, screened):
    krow_count = lax.axis_size("krow")
    momentum_column_count = lax.axis_size("kcol")
    orbitals = green.shape[4]
    slice_len = orbitals * green.shape[5] // (krow_count * momentum_column_count)
    blocks = green.reshape(green.shape[:4] + (krow_count, momentum_column_count, slice_len))
    weights = screened.reshape(screened.shape[0], screened.shape[1], 1, 1, screened.shape[2])
    gathered = lax.all_to_all(
        lax.all_to_all(blocks, "krow", split_axis=4, concat_axis=2, tiled=True),
        "kcol",
        split_axis=5,
        concat_axis=3,
        tiled=True,
    )
    middle = whole_local(gathered, weights)
    partway = lax.all_to_all(middle, "krow", split_axis=2, concat_axis=4, tiled=True)
    returned = lax.all_to_all(partway, "kcol", split_axis=3, concat_axis=5, tiled=True)
    sigma = returned.reshape(green.shape)
    green_real = green[:, 0]
    green_imag = green[:, 1]
    self_energy_real = sigma[:, 0]
    self_energy_imaginary = sigma[:, 1]
    kern_real = (
        matmul_batch(green_real, self_energy_real) - matmul_batch(green_imag, self_energy_imaginary)
    ).astype(jnp.bfloat16)
    kern_imag = (
        matmul_batch(green_real, self_energy_imaginary) + matmul_batch(green_imag, self_energy_real)
    ).astype(jnp.bfloat16)
    corr_real = matmul_batch(kern_real, green_real) - matmul_batch(kern_imag, green_imag)
    corr_imag = matmul_batch(kern_real, green_imag) + matmul_batch(kern_imag, green_real)
    dressed_real = green_real.astype(jnp.float32) + corr_real / orbitals
    dressed_imag = green_imag.astype(jnp.float32) + corr_imag / orbitals
    dressed = jnp.stack((dressed_real, dressed_imag), 1).astype(jnp.bfloat16)
    return (sigma, dressed)


def choose(green, screened):
    devices = lax.axis_size("krow") * lax.axis_size("kcol")
    orbitals = green.shape[4]
    shaped = lax.axis_size("krow") % (2 * SPLIT_X * CORES) == 0 and lax.axis_size("kcol") > 1
    if shaped and orbitals % (devices * SUBLANES) == 0 and orbitals % LANES == 0:
        return exchange_in_kernel(green, screened)
    return per_device(green, screened)


def solution(mesh):
    placed = (P(None, None, "krow", "kcol", None, None), P(None, None, ("krow", "kcol")))
    return jax.shard_map(
        choose,
        mesh=mesh,
        in_specs=placed,
        out_specs=(
            P(None, None, "krow", "kcol", None, None),
            P(None, None, "krow", "kcol", None, None),
        ),
        check_vma=False,
    )
```

```python
import functools
import math

import jax
import jax.numpy as jnp
from jax import lax
from jax.experimental import pallas as pl
from jax.experimental.pallas import tpu as pltpu
from jax.sharding import PartitionSpec as P

SUBLANES = 8
LANES = 128


def turn(values, count, size, sign):
    real, imag = values
    count = count * sign % size
    if count * 8 % size == 0:
        eighth = count * 8 // size
        half = math.sqrt(0.5)
        if eighth == 0:
            return real, imag
        if eighth == 2:
            return -imag, real
        if eighth == 4:
            return -real, -imag
        if eighth == 6:
            return imag, -real
        if eighth == 1:
            return (real - imag) * half, (real + imag) * half
        if eighth == 3:
            return (real + imag) * -half, (real - imag) * half
        if eighth == 5:
            return (imag - real) * half, (real + imag) * -half
        return (real + imag) * half, (imag - real) * half
    angle = 2.0 * math.pi * count / size
    cosine, sine = math.cos(angle), math.sin(angle)
    return real * cosine - imag * sine, real * sine + imag * cosine


def transform(values, sign):
    size = len(values)
    if size == 1:
        return values
    if size % 2:
        out = []
        for target in range(size):
            terms = [turn(v, target * source, size, sign) for source, v in enumerate(values)]
            out.append((sum(t[0] for t in terms), sum(t[1] for t in terms)))
        return out
    even = transform(values[0::2], sign)
    odd = transform(values[1::2], sign)
    low, high = [], []
    for t in range(size // 2):
        real, imag = turn(odd[t], t, size, sign)
        low.append((even[t][0] + real, even[t][1] + imag))
        high.append((even[t][0] - real, even[t][1] - imag))
    return low + high


CORES = 2
SPLIT_X = 2
PILLAR_ORDER = ((1, 0, 2, 3), (2, 0, 3, 1), (0, 1, 3, 2), (0, 2, 1, 3))


def corrected(g_real, g_imag, s_real, s_imag):
    def times(left, right):
        return jnp.dot(left, right, preferred_element_type=jnp.float32)

    kern_real = (times(g_real, s_real) - times(g_imag, s_imag)).astype(jnp.bfloat16)
    kern_imag = (times(g_real, s_imag) + times(g_imag, s_real)).astype(jnp.bfloat16)
    corr_real = times(kern_real, g_real) - times(kern_imag, g_imag)
    corr_imag = times(kern_real, g_imag) + times(kern_imag, g_real)
    share = 1.0 / g_real.shape[-1]
    return (
        (g_real.astype(jnp.float32) + corr_real * share).astype(jnp.bfloat16),
        (g_imag.astype(jnp.float32) + corr_imag * share).astype(jnp.bfloat16),
    )


def kernel(
    grid_dims, mesh_dims, rows,
    green_far, weights_far, green, sigma, dressed,
    weights, arrived, results, middle, pair_weights,
    load_sems, out_sems, in_sems, back_out_sems, back_in_sems, near_sems, all_in,
):
    one, two = grid_dims
    row_count, column_count = mesh_dims
    devices = row_count * column_count
    energies, _, local, orbitals, _ = green.shape
    local_one, local_two = one // row_count, two // column_count
    my_row, my_column = lax.axis_index("krow"), lax.axis_index("kcol")
    me = my_row * column_count + my_column

    plane_rows = SPLIT_X * CORES
    layers = row_count // plane_rows
    half = layers // 2
    plane = plane_rows * column_count
    pillars = SPLIT_X * column_count
    z = lax.div(my_row, plane_rows)
    x = lax.rem(lax.div(my_row, CORES), SPLIT_X)
    core = lax.rem(my_row, CORES)
    y = my_column
    pillar = x * column_count + y

    def at_place(z_, x_, core_, y_):
        return ((z_ * SPLIT_X + x_) * CORES + core_, y_)

    def flat_of(place):
        return place[0] * column_count + place[1]

    def signal(sem, place):
        pl.semaphore_signal(
            sem, inc=1, device_id=place, device_id_type=pl.DeviceIdType.MESH
        )

    def strip(owner):
        return pl.ds(pl.multiple_of(owner * rows, rows), rows)

    def load(e):
        return pltpu.make_async_copy(green_far.at[e], green.at[e], load_sems.at[e])

    load_weights = pltpu.make_async_copy(weights_far, weights, load_sems.at[energies])

    barrier = pltpu.get_barrier_semaphore()
    last_place = (z == layers - 1) & (x == SPLIT_X - 1) & (y == column_count - 1)

    @pl.when(last_place)
    def _():
        signal(barrier, at_place(z, x, 1 - core, y))

    def flag(condition):
        return jnp.where(condition, 1, 0)

    heard = CORES * (flag(x > 0) + flag(y > 0) + flag(z > 0)) + flag(last_place) * (CORES - 1)

    @pl.when(heard > 0)
    def _():
        pl.semaphore_wait(barrier, heard)

    for c in range(CORES):
        @pl.when(z < layers - 1)
        def _():
            signal(barrier, at_place(z + 1, x, c, y))

        @pl.when(z >= half)
        def _():
            signal(near_sems.at[z - half], at_place(half - 1, x, c, y))

        @pl.when(x < SPLIT_X - 1)
        def _():
            signal(barrier, at_place(z, x + 1, c, y))

        @pl.when(y < column_count - 1)
        def _():
            signal(barrier, at_place(z, x, c, y + 1))

    @pl.when(last_place)
    def _():
        @pl.loop(1, row_count // CORES * column_count)
        def _(step):
            chip = row_count // CORES * column_count - 1 - step
            signal(all_in, (lax.div(chip, column_count) * CORES + core, lax.rem(chip, column_count)))

    def send(e, place):
        peer = flat_of(place)
        pltpu.make_async_remote_copy(
            src_ref=green_far.at[e, :, :, strip(peer), :],
            dst_ref=arrived.at[e, me],
            send_sem=out_sems.at[e],
            recv_sem=in_sems.at[e],
            device_id=place,
            device_id_type=pl.DeviceIdType.MESH,
        ).start()

    def send_pillar(z_):
        @pl.loop(0, energies)
        def _(e):
            for c in range(CORES):
                send(e, at_place(z_, x, lax.rem(core + c, CORES), y))

    @pl.when(z == half)
    def _():
        @pl.loop(0, half)
        def _(step):
            send_pillar(half - 1 - step)

    for e in range(energies):
        load(e).start()
    load_weights.start()

    @pl.when(z == half - 1)
    def _():
        @pl.loop(0, layers - half)
        def _(step):
            pl.semaphore_wait(near_sems.at[step], CORES)
            send_pillar(half + step)

    @pl.when(jnp.logical_not(last_place))
    def _():
        pl.semaphore_wait(all_in, 1)

    middle_layer = (z == half) | (z == half - 1)

    def next_pillar(turn_):
        if pillars != len(PILLAR_ORDER):
            return lax.rem(pillar + 1 + turn_, pillars)
        to = 0
        for source, order in enumerate(PILLAR_ORDER):
            for when, target_ in enumerate(order):
                to = to + jnp.where((pillar == source) & (turn_ == when), target_, 0)
        return to

    def each_peer(first_round, body):
        @pl.loop(0, pillars * layers)
        def _(n):
            paired = (z >= half) & (pillar > 0)
            step = jnp.where(paired, lax.rem(lax.div(n, 2), layers), lax.rem(n, layers))
            turn_ = jnp.where(paired, lax.div(n, 2 * layers) * 2 + lax.rem(n, 2), lax.div(n, layers))
            to = next_pillar(turn_)
            own = to == pillar
            z_ = lax.rem(z + step, layers)
            across = (z_ >= half) != (z >= half)
            done = flag(own & (step == 0))
            if first_round:
                done = jnp.where(own & middle_layer & across, CORES, done)

            @pl.loop(done, CORES)
            def _(c):
                body(at_place(
                    z_, lax.div(to, column_count), lax.rem(core + c, CORES),
                    lax.rem(to, column_count),
                ))

    @pl.loop(0, energies)
    def _(e):
        each_peer(True, lambda place: send(e, place))

    def wait_all(part, sem):
        pltpu.make_async_copy(part, part, sem).wait()

    def others(buffer, e):
        return buffer.at[e, pl.ds(0, devices - 1)]

    def slot(k1, k2):
        return (
            (k1 // local_one) * column_count + k2 // local_two,
            (k1 % local_one) * local_two + k2 % local_two,
        )

    scale = -1.0 / (one * two)
    load_weights.wait()

    @pl.loop(0, one)
    def _(r1):
        for r2 in range(two):
            for row in range(rows):
                part = weights[r1, r2:r2 + 1, row * orbitals:(row + 1) * orbitals]
                pair_weights[r1, r2, row:row + 1, :] = part * scale

    def transform_energy(e):
        load(e).wait()
        wait_all(others(arrived, e), in_sems.at[e])
        arrived[e, me] = green[e, :, :, strip(me), :]

        @pl.loop(0, orbitals // LANES)
        def _(h):
            lanes = pl.ds(pl.multiple_of(h * LANES, LANES), LANES)
            for k2 in range(two):
                values = []
                for k1 in range(one):
                    s, at = slot(k1, k2)
                    values.append(tuple(
                        arrived[e, s, c, at, :, lanes].astype(jnp.float32) for c in range(2)
                    ))
                for r1, v in enumerate(transform(values, 1)):
                    middle[r1, k2, 0] = v[0]
                    middle[r1, k2, 1] = v[1]
            for r1 in range(one):
                values = transform([(middle[r1, k2, 0], middle[r1, k2, 1]) for k2 in range(two)], 1)
                for r2 in range(two):
                    weight = pair_weights[r1, r2, :, lanes]
                    values[r2] = (values[r2][0] * weight, values[r2][1] * weight)
                for k2, v in enumerate(transform(values, -1)):
                    middle[r1, k2, 0] = v[0]
                    middle[r1, k2, 1] = v[1]
            for k2 in range(two):
                values = [(middle[r1, k2, 0], middle[r1, k2, 1]) for r1 in range(one)]
                for k1, v in enumerate(transform(values, -1)):
                    s, at = slot(k1, k2)
                    for c in range(2):
                        results[e, s, c, at, :, lanes] = v[c].astype(jnp.bfloat16)

    def send_back(e):
        def one_send(place):
            pltpu.make_async_remote_copy(
                src_ref=results.at[e, flat_of(place)],
                dst_ref=sigma.at[e, :, :, strip(me), :],
                send_sem=back_out_sems.at[e],
                recv_sem=back_in_sems.at[e],
                device_id=place,
                device_id_type=pl.DeviceIdType.MESH,
            ).start()

        each_peer(False, one_send)

    last = energies - 1

    @pl.loop(0, energies)
    def _(e):
        transform_energy(e)

        send_back(e)
        sigma[e, :, :, strip(me), :] = results[e, me]

    @pl.loop(0, last)
    def _(e):
        wait_all(others(results, e), back_in_sems.at[e])

        @pl.loop(0, local)
        def _(at):
            real, imag = corrected(
                green[e, 0, at], green[e, 1, at], sigma[e, 0, at], sigma[e, 1, at]
            )
            dressed[e, 0, at] = real
            dressed[e, 1, at] = imag

    @pl.loop(0, last)
    def _(e):
        wait_all(others(arrived, e), out_sems.at[e])
        wait_all(others(results, e), back_out_sems.at[e])

    wait_all(others(arrived, last), out_sems.at[last])
    wait_all(others(results, last), back_out_sems.at[last])
    wait_all(others(results, last), back_in_sems.at[last])


def finish(green, sigma, dressed, sigma_far, dressed_far, piece, sems):
    energies, _, local, _, _ = green.shape
    last = energies - 1
    copies = [
        pltpu.make_async_copy(sigma, sigma_far, sems.at[local]),
        pltpu.make_async_copy(
            dressed.at[pl.ds(0, last)], dressed_far.at[pl.ds(0, last)], sems.at[local + 1]
        ),
    ]
    for copy in copies:
        copy.start()
    for at in range(local):
        piece[at, 0], piece[at, 1] = corrected(
            green[last, 0, at], green[last, 1, at], sigma[last, 0, at], sigma[last, 1, at]
        )
        copies.append(
            pltpu.make_async_copy(piece.at[at], dressed_far.at[last, :, at], sems.at[at])
        )
        copies[-1].start()
    for copy in copies:
        copy.wait()


def exchange_in_kernel(green, screened):
    mesh_dims = (lax.axis_size("krow"), lax.axis_size("kcol"))
    devices = mesh_dims[0] * mesh_dims[1]
    energies, _, local_one, local_two, orbitals, _ = green.shape
    grid_dims = screened.shape[:2]
    rows = orbitals // devices
    local = local_one * local_two
    layers = mesh_dims[0] // (SPLIT_X * CORES)
    flat = (energies, 2, local, orbitals, orbitals)
    block = (energies, devices, 2, local, rows, orbitals)
    vmem = pl.BlockSpec(memory_space=pltpu.VMEM)
    far = pl.BlockSpec(memory_space=pltpu.HBM)
    held = pl.pallas_call(
        functools.partial(kernel, grid_dims, mesh_dims, rows),
        out_shape=[pltpu.VMEM(flat, jnp.bfloat16)] * 3,
        in_specs=[far, far],
        out_specs=[vmem] * 3,
        scratch_shapes=[
            pltpu.VMEM(screened.shape, jnp.float32),
            pltpu.VMEM(block, jnp.bfloat16),
            pltpu.VMEM(block, jnp.bfloat16),
            pltpu.VMEM(grid_dims + (2, rows, LANES), jnp.float32),
            pltpu.VMEM(grid_dims + (rows, orbitals), jnp.float32),
            pltpu.SemaphoreType.DMA((energies + 1,)),
            pltpu.SemaphoreType.DMA((energies,)),
            pltpu.SemaphoreType.DMA((energies,)),
            pltpu.SemaphoreType.DMA((energies,)),
            pltpu.SemaphoreType.DMA((energies,)),
            pltpu.SemaphoreType.REGULAR((layers - layers // 2,)),
            pltpu.SemaphoreType.REGULAR,
        ],
        compiler_params=pltpu.CompilerParams(
            collective_id=0, has_side_effects=True, vmem_limit_bytes=15 * math.prod(block)
        ),
    )(*(
        pltpu.with_memory_space_constraint(v, pltpu.HBM) for v in (green.reshape(flat), screened)
    ))
    sigma, dressed = pl.pallas_call(
        finish,
        out_shape=[jax.ShapeDtypeStruct(flat, jnp.bfloat16)] * 2,
        in_specs=[vmem] * 3,
        out_specs=[far] * 2,
        scratch_shapes=[
            pltpu.VMEM((local, 2, orbitals, orbitals), jnp.bfloat16),
            pltpu.SemaphoreType.DMA((local + 2,)),
        ],
        compiler_params=pltpu.CompilerParams(vmem_limit_bytes=8 * math.prod(block)),
    )(*held)
    return sigma.reshape(green.shape), dressed.reshape(green.shape)


full_turn = 2.0 * math.pi


def phase_tables(length, forward):
    step_counter = jnp.arange(length, dtype=jnp.int32)
    product = step_counter[:, None] * step_counter[None, :] % length
    angles = full_turn * product.astype(jnp.float32) / length
    if forward:
        return (jnp.cos(angles) / length, jnp.sin(angles) / length)
    return (jnp.cos(angles), -jnp.sin(angles))


def apply_over_axis(matrix, values, along_dim):
    letters = "abcdefgh"[: values.ndim]
    target = letters[:along_dim] + "z" + letters[along_dim + 1 :]
    formula = "z" + letters[along_dim] + "," + letters + "->" + target
    return jnp.einsum(formula, matrix, values, precision=lax.Precision.HIGHEST)


def complex_along(state, cosine, sine, along_dim):
    real_part, imag_part = state
    out_real = apply_over_axis(cosine, real_part, along_dim) - apply_over_axis(
        sine, imag_part, along_dim
    )
    out_imag = apply_over_axis(sine, real_part, along_dim) + apply_over_axis(
        cosine, imag_part, along_dim
    )
    return (out_real, out_imag)


def weigh_back(state, weights, lead_one, lead_two):
    state = (-weights * state[0], -weights * state[1])
    cos_one, sin_one = phase_tables(lead_one, False)
    state = complex_along(state, cos_one, sin_one, 1)
    cos_two, sin_two = phase_tables(lead_two, False)
    state = complex_along(state, cos_two, sin_two, 2)
    return jnp.stack(state, 1).astype(jnp.bfloat16)


def whole_local(pieces, weights):
    state = (pieces[:, 0].astype(jnp.float32), pieces[:, 1].astype(jnp.float32))
    cos_two, sin_two = phase_tables(pieces.shape[3], True)
    state = complex_along(state, cos_two, sin_two, 2)
    cos_one, sin_one = phase_tables(pieces.shape[2], True)
    state = complex_along(state, cos_one, sin_one, 1)
    return weigh_back(state, weights, pieces.shape[2], pieces.shape[3])


def matmul_batch(left, right):
    return jnp.einsum("eklij,ekljm->eklim", left, right, preferred_element_type=jnp.float32)


def per_device(green, screened):
    krow_count = lax.axis_size("krow")
    momentum_column_count = lax.axis_size("kcol")
    orbitals = green.shape[4]
    slice_len = orbitals * green.shape[5] // (krow_count * momentum_column_count)
    blocks = green.reshape(green.shape[:4] + (krow_count, momentum_column_count, slice_len))
    weights = screened.reshape(screened.shape[0], screened.shape[1], 1, 1, screened.shape[2])
    gathered = lax.all_to_all(
        lax.all_to_all(blocks, "krow", split_axis=4, concat_axis=2, tiled=True),
        "kcol",
        split_axis=5,
        concat_axis=3,
        tiled=True,
    )
    middle = whole_local(gathered, weights)
    partway = lax.all_to_all(middle, "krow", split_axis=2, concat_axis=4, tiled=True)
    returned = lax.all_to_all(partway, "kcol", split_axis=3, concat_axis=5, tiled=True)
    sigma = returned.reshape(green.shape)
    green_real = green[:, 0]
    green_imag = green[:, 1]
    self_energy_real = sigma[:, 0]
    self_energy_imaginary = sigma[:, 1]
    kern_real = (
        matmul_batch(green_real, self_energy_real) - matmul_batch(green_imag, self_energy_imaginary)
    ).astype(jnp.bfloat16)
    kern_imag = (
        matmul_batch(green_real, self_energy_imaginary) + matmul_batch(green_imag, self_energy_real)
    ).astype(jnp.bfloat16)
    corr_real = matmul_batch(kern_real, green_real) - matmul_batch(kern_imag, green_imag)
    corr_imag = matmul_batch(kern_real, green_imag) + matmul_batch(kern_imag, green_real)
    dressed_real = green_real.astype(jnp.float32) + corr_real / orbitals
    dressed_imag = green_imag.astype(jnp.float32) + corr_imag / orbitals
    dressed = jnp.stack((dressed_real, dressed_imag), 1).astype(jnp.bfloat16)
    return (sigma, dressed)


def choose(green, screened):
    devices = lax.axis_size("krow") * lax.axis_size("kcol")
    orbitals = green.shape[4]
    shaped = lax.axis_size("krow") % (2 * SPLIT_X * CORES) == 0 and lax.axis_size("kcol") > 1
    if shaped and orbitals % (devices * SUBLANES) == 0 and orbitals % LANES == 0:
        return exchange_in_kernel(green, screened)
    return per_device(green, screened)


def solution(mesh):
    placed = (P(None, None, "krow", "kcol", None, None), P(None, None, ("krow", "kcol")))
    return jax.shard_map(
        choose,
        mesh=mesh,
        in_specs=placed,
        out_specs=(
            P(None, None, "krow", "kcol", None, None),
            P(None, None, "krow", "kcol", None, None),
        ),
        check_vma=False,
    )
```
